32 devices in a mesh: replica: 2 (over core), model: 4 (over y, x), shift: 4 (over z).
Axes of the slice: x: 2, y: 2, z: 4, core: 2. Of those that a mesh axis runs over, the one named last changes fastest.
Arguments:
- partial_gate: float32 [8, 1024, 3072], P(('shift', 'replica'), None, 'model'), parts along dimension 0, may hold values from -0.875 to 0.875
- partial_up: float32 [8, 1024, 3072], P(('shift', 'replica'), None, 'model'), parts along dimension 0, may hold values from -0.875 to 0.875
- partial_down: float32 [8, 3072, 1024], P(('shift', 'replica'), 'model'), parts along dimension 0, may hold values from -0.875 to 0.875
- partial_norm: float32 [8, 1024], P(('shift', 'replica')), parts along dimension 0, may hold values from -8 to 8
- master_gate: float32 [4096, 3072], P(('shift', 'replica'), 'model'), parts along dimension 0, may hold values from -0.25 to 0.25
- master_up: float32 [4096, 3072], P(('shift', 'replica'), 'model'), parts along dimension 0, may hold values from -0.25 to 0.25
- master_down: float32 [12288, 1024], P(('shift', 'model'), 'replica'), parts along dimension 0, may hold values from -0.15625 to 0.15625
- master_norm: float32 [4096], P(('shift', 'replica')), parts along dimension 0, may hold values from 0.25 to 1.75
- memory_gate: float32 [4096, 3072], P(('shift', 'replica'), 'model'), parts along dimension 0, may hold values from -0.1875 to 0.1875
- memory_up: float32 [4096, 3072], P(('shift', 'replica'), 'model'), parts along dimension 0, may hold values from -0.1875 to 0.1875
- memory_down: float32 [12288, 1024], P(('shift', 'model'), 'replica'), parts along dimension 0, may hold values from -0.109375 to 0.109375
- memory_norm: float32 [4096], P(('shift', 'replica')), parts along dimension 0, may hold values from -1.75 to 1.75
Outputs:
- compute_gate: bfloat16 [4096, 3072], P('shift', 'model'), parts along dimension 0
- compute_up: bfloat16 [4096, 3072], P('shift', 'model'), parts along dimension 0
- compute_down: bfloat16 [12288, 1024], P(('shift', 'model')), parts along dimension 0
- compute_norm: bfloat16 [4096], P('shift'), parts along dimension 0
- stepped_gate: float32 [4096, 3072], P(('shift', 'replica'), 'model'), parts along dimension 0
- stepped_up: float32 [4096, 3072], P(('shift', 'replica'), 'model'), parts along dimension 0
- stepped_down: float32 [12288, 1024], P(('shift', 'model'), 'replica'), parts along dimension 0
- stepped_norm: float32 [4096], P(('shift', 'replica')), parts along dimension 0
- state_new_gate: float32 [4096, 3072], P(('shift', 'replica'), 'model'), parts along dimension 0
- state_new_up: float32 [4096, 3072], P(('shift', 'replica'), 'model'), parts along dimension 0
- state_new_down: float32 [12288, 1024], P(('shift', 'model'), 'replica'), parts along dimension 0
- state_new_norm: float32 [4096], P(('shift', 'replica')), parts along dimension 0
The draws below stay inside these ranges and needn't reach their ends.
There are 4 independent parts, one for each index of `shift`. The reference program is written for one: setup_inputs(seed, part) draws one part's arguments, and reference() takes and returns one part's arrays. A program takes and returns all parts, laid end to end along the dimension named above; each array names one. Nothing has to cross between parts.
All inputs are finite; a program needn't handle non-finite values.
Results may differ from the reference program's by a relative error of at most 0.001.
Values may be sent and summed in bfloat16 or wider, within the bound.
A program may use at most 128 MiB of HBM per device.

```python
import jax
import jax.numpy as jnp
from jax import lax

WIDTH = 1024
INNER = 3072
REPLICAS = 2


def spiked(drawn, own_key, source, target, parts, factor):
    owner, partner = [(jnp.arange(drawn.shape[axis_at]) // (drawn.shape[axis_at] // parts)).reshape([-1 if axis == axis_at else 1 for axis in range(drawn.ndim)]) for axis_at in (source, target)]
    chosen = jax.random.permutation(own_key, parts)[partner]
    strong = (owner == chosen) | (owner == (partner + parts // 2) % parts)
    return jnp.where(strong, factor * drawn, drawn)


def steps_of(stream_key, dims, cuts, smallest, high):
    def one(position, blocks):
        steps = jax.random.uniform(jax.random.fold_in(jax.random.fold_in(stream_key, 6), position), (blocks,), jnp.float32, smallest / len(cuts), high / len(cuts))
        return jnp.repeat(jnp.exp(steps), dims[position] // blocks).reshape((-1,) + (1,) * (len(dims) - position - 1))

    loudness = one(*cuts[0])
    for cut in cuts[1:]:
        loudness = loudness * one(*cut)
    return loudness


def scatter_about(key, dims, deviation, most, pieces=(), dtype=jnp.bfloat16):
    factor_of = steps_of(key, dims, pieces, -0.22, 0.18) if pieces else 1.0
    values = jax.random.normal(key, dims, jnp.float32) * deviation * factor_of
    return jnp.minimum(jnp.maximum(values, -most), most).astype(dtype)


def noise_with(key, dims, scale, limit, split, heavy, kind=jnp.bfloat16):
    entries = scale * jax.random.normal(key, dims, jnp.float32)
    if split:
        entries = entries * steps_of(key, dims, split, -0.22, 0.18)
    return jnp.clip(spiked(entries, jax.random.fold_in(key, 3), *heavy), -limit, limit).astype(kind)


def setup_inputs(seed: int = 0, part: int = 0) -> dict:
    keys = jax.random.split(jax.random.key(seed), 13)
    part_splits = jax.random.split(jax.random.fold_in(keys[12], part), 13)
    partial_gate = noise_with(part_splits[0], (REPLICAS, WIDTH, INNER), 0.1, 0.875, ((0, 2), (2, 4)), (0, 1, 2, 2.0), jnp.float32)
    partial_up = noise_with(part_splits[1], (REPLICAS, WIDTH, INNER), 0.1, 0.875, ((0, 2), (2, 4)), (0, 1, 2, 2.0), jnp.float32)
    partial_down = noise_with(part_splits[2], (REPLICAS, INNER, WIDTH), 0.1, 0.875, ((0, 2), (1, 4)), (0, 2, 2, 2.0), jnp.float32)
    partial_norm = noise_with(part_splits[3], (REPLICAS, WIDTH), 1.0, 8.0, ((0, 2),), (0, 1, 2, 2.0), jnp.float32)
    master_gate = noise_with(part_splits[4], (WIDTH, INNER), WIDTH ** -0.5, 0.25, ((0, 2), (1, 4)), (1, 0, 4, 2.0), jnp.float32)
    master_up = noise_with(part_splits[5], (WIDTH, INNER), WIDTH ** -0.5, 0.25, ((0, 2), (1, 4)), (1, 0, 4, 2.0), jnp.float32)
    master_down = noise_with(part_splits[6], (INNER, WIDTH), INNER ** -0.5, 0.15625, ((0, 4), (1, 2)), (0, 1, 4, 2.0), jnp.float32)
    master_norm = jnp.clip(1.0 + 0.15 * jax.random.normal(part_splits[7], (WIDTH,), jnp.float32), 0.25, 1.75)
    memory_gate = scatter_about(part_splits[8], (WIDTH, INNER), WIDTH ** -0.5, 0.1875, ((0, 2), (1, 4)), jnp.float32)
    memory_up = scatter_about(part_splits[9], (WIDTH, INNER), WIDTH ** -0.5, 0.1875, ((0, 2), (1, 4)), jnp.float32)
    memory_down = scatter_about(part_splits[10], (INNER, WIDTH), INNER ** -0.5, 0.109375, ((0, 4), (1, 2)), jnp.float32)
    memory_norm = scatter_about(part_splits[11], (WIDTH,), 0.3, 1.75, ((0, 2),), jnp.float32)
    return {"partial_gate": partial_gate, "partial_up": partial_up, "partial_down": partial_down, "partial_norm": partial_norm, "master_gate": master_gate, "master_up": master_up, "master_down": master_down, "master_norm": master_norm, "memory_gate": memory_gate, "memory_up": memory_up, "memory_down": memory_down, "memory_norm": memory_norm}


learn_rate = 0.5
hold_rate = 0.9

def reference(partial_gate, partial_up, partial_down, partial_norm, master_gate, master_up, master_down, master_norm, memory_gate, memory_up, memory_down, memory_norm):
    mean_gate = lax.optimization_barrier(jnp.sum(partial_gate.astype(jnp.float32), axis=0)) * REPLICAS ** (-0.5)
    mean_up = lax.optimization_barrier(jnp.sum(partial_up.astype(jnp.float32), axis=0)) * REPLICAS ** (-0.5)
    mean_down = lax.optimization_barrier(jnp.sum(partial_down.astype(jnp.float32), axis=0)) * REPLICAS ** (-0.5)
    mean_norm = lax.optimization_barrier(jnp.sum(partial_norm.astype(jnp.float32), axis=0)) * REPLICAS ** (-0.5)
    ratio_gate = jnp.sqrt(lax.optimization_barrier(jnp.sum(master_gate * master_gate, axis=1, keepdims=True))) * lax.rsqrt(lax.optimization_barrier(jnp.sum(mean_gate * mean_gate, axis=1, keepdims=True)) + 1e-06)
    mean_gate = mean_gate * ratio_gate
    ratio_up = jnp.sqrt(lax.optimization_barrier(jnp.sum(master_up * master_up, axis=1, keepdims=True))) * lax.rsqrt(lax.optimization_barrier(jnp.sum(mean_up * mean_up, axis=1, keepdims=True)) + 1e-06)
    mean_up = mean_up * ratio_up
    ratio_down = jnp.sqrt(lax.optimization_barrier(jnp.sum(master_down * master_down, axis=0, keepdims=True))) * lax.rsqrt(lax.optimization_barrier(jnp.sum(mean_down * mean_down, axis=0, keepdims=True)) + 1e-06)
    mean_down = mean_down * ratio_down
    state_new_gate = hold_rate * memory_gate + mean_gate
    stepped_gate = master_gate - learn_rate * state_new_gate
    state_new_up = hold_rate * memory_up + mean_up
    stepped_up = master_up - learn_rate * state_new_up
    state_new_down = hold_rate * memory_down + mean_down
    stepped_down = master_down - learn_rate * state_new_down
    state_new_norm = hold_rate * memory_norm + mean_norm
    stepped_norm = master_norm - learn_rate * state_new_norm
    compute_gate = stepped_gate.astype(jnp.bfloat16)
    compute_up = stepped_up.astype(jnp.bfloat16)
    compute_down = stepped_down.astype(jnp.bfloat16)
    compute_norm = stepped_norm.astype(jnp.bfloat16)
    return (compute_gate, compute_up, compute_down, compute_norm, stepped_gate, stepped_up, stepped_down, stepped_norm, state_new_gate, state_new_up, state_new_down, state_new_norm)
```

```python
import functools
import math

import jax
import jax.numpy as jnp
from jax import lax
from jax.experimental import pallas as pl
from jax.experimental.pallas import tpu as pltpu
from jax.sharding import PartitionSpec as P

learn_rate = 0.5
hold_rate = 0.9
MESH = pl.DeviceIdType.MESH
LANES = 128
CODE_SCALE = 2.0**13


def cut(ref, axis, start, size):
    return ref.at[pl.ds(start, size), :] if axis == 0 else ref.at[:, pl.ds(start, size)]


def code(x):
    x = x * CODE_SCALE
    x = x * x * x
    return (x * x * x).astype(jnp.bfloat16)


def decode(y):
    y = y.astype(jnp.float32)
    size = jnp.maximum(jnp.abs(y), 2.0**-126)
    return y * lax.exp2(lax.log2(size) * (-8 / 9) - math.log2(CODE_SCALE))


def kernel(m, axes, *refs):
    refs = list(refs)
    take = lambda count: [refs.pop(0) for _ in range(count)]
    t = len(axes)
    partial, (partial_norm,) = take(t), take(1)
    master_hbm, (master_norm,) = take(t), take(1)
    memory_hbm, (memory_norm,) = take(t), take(1)
    compute, (compute_norm,) = take(t), take(1)
    stepped, (stepped_norm,) = take(t), take(1)
    state, (state_norm,) = take(t), take(1)
    other, sent, got, memory = take(t), take(t), take(t), take(t)
    master, mean = stepped, state
    mean_n, got_n, master_n, memory_n, whole_n, line_n = take(6)
    line, line_got, fold, tile = take(4)
    load_sem, part_send, part_recv, comp_send, comp_recv = take(5)
    line_send, line_recv, norm_load_sem, norm_send, norm_recv, ready = take(6)

    me = lax.axis_index("replica")
    at = lax.axis_index("model")
    peer = 1 - me
    rate = 2 ** (-0.5)
    mates = [lax.rem(at + k, m) for k in range(1, m)]

    chunks = []
    for which, axis in enumerate(axes):
        share = mean[which].shape[axis]
        chunks += [(which, c) for c in range(share // LANES)]
    chunks.insert(0, chunks.pop(chunks.index((t - 1, 0))))
    count, lead = len(chunks), 4

    def load(kind, number):
        which, c = chunks[number]
        axis = axes[which]
        share = mean[which].shape[axis]
        source = (partial[which].at[0], partial[which].at[0], master_hbm[which], memory_hbm[which])
        target = (other, mean, master, memory)[kind][which]
        start = ((peer, me)[kind] * share if kind < 2 else 0) + c * LANES
        start = pl.multiple_of(start, LANES)
        return pltpu.make_async_copy(
            cut(source[kind], axis, start, LANES),
            cut(target, axis, c * LANES, LANES),
            load_sem.at[(number - lead) % (count + lead) if kind == 0 else number],
        )

    def wait_loads(number):
        size = (3 if number + lead < count else 2) * LANES
        pltpu.make_async_copy(
            master_hbm[0].at[pl.ds(0, size), :],
            master[0].at[pl.ds(0, size), :],
            load_sem.at[number],
        ).wait()

    share_n = mean_n.shape[1]
    own_n = pl.ds(pl.multiple_of(me * share_n, LANES), share_n)
    norm_loads = [
        pltpu.make_async_copy(partial_norm.at[:, own_n], mean_n, norm_load_sem.at[0]),
        pltpu.make_async_copy(master_norm, master_n, norm_load_sem.at[1]),
        pltpu.make_async_copy(memory_norm, memory_n, norm_load_sem.at[2]),
    ]

    def to_peer(source, target, send, recv):
        return pltpu.make_async_remote_copy(
            src_ref=source,
            dst_ref=target,
            send_sem=send,
            recv_sem=recv,
            device_id={"replica": peer},
            device_id_type=MESH,
        )

    def part_copy(number):
        which, c = chunks[number]
        return to_peer(
            sent[which].at[c], got[which].at[c], part_send.at[which], part_recv.at[number]
        )

    def comp_copy(number):
        which, c = chunks[number]
        axis = axes[which]
        share = mean[which].shape[axis]
        mine = cut(compute[which], axis, pl.multiple_of(me * share + c * LANES, LANES), LANES)
        return to_peer(mine, mine, comp_send.at[which], comp_recv.at[which])

    def comp_half(which):
        axis = axes[which]
        share = mean[which].shape[axis]
        mine = cut(compute[which], axis, pl.multiple_of(me * share, LANES), share)
        return to_peer(mine, mine, comp_send.at[which], comp_recv.at[which])

    peer_n = pl.ds(pl.multiple_of(peer * share_n, LANES), share_n)
    part_norm_copy = to_peer(partial_norm.at[:, peer_n], got_n, norm_send.at[0], norm_recv.at[0])
    whole_norm_copy = to_peer(
        whole_n.at[:, own_n], whole_n.at[:, own_n], norm_send.at[1], norm_recv.at[1]
    )

    def to_mate(source, target, recv, k):
        return pltpu.make_async_remote_copy(
            src_ref=source,
            dst_ref=target,
            send_sem=line_send.at[0],
            recv_sem=recv,
            device_id={"model": mates[k]},
            device_id_type=MESH,
        )

    def line_copy(number, k):
        return to_mate(line.at[number], line_got.at[number, k], line_recv.at[number], k)

    def blocks(number):
        which, c = chunks[number]
        rows, columns = mean[which].shape
        if axes[which] == 0:
            height = 32
            for b in range(LANES // height):
                inside = (pl.ds(b * height, height), slice(None))
                yield inside, (pl.ds(c * LANES + b * height, height), slice(None))
        else:
            height = next(h for h in (128, 64, 32, 16, 8) if rows % h == 0)
            for b in range(rows // height):
                r = pl.ds(b * height, height)
                yield (r, slice(None)), (r, pl.ds(c * LANES, LANES))

    def prepare(number):
        which, c = chunks[number]
        for inside, block in blocks(number):
            sent[which][(c, *inside)] = code(other[which][block])

    def squares(number, row, block_of):
        which, c = chunks[number]
        if axes[which] == 0:
            for inside, block in blocks(number):
                value = block_of(inside, block)
                value = value * value
                fold[number % 2, row, inside[0], :] = sum(
                    value[:, j : j + LANES] for j in range(0, value.shape[1], LANES)
                )
        else:
            total = jnp.zeros((8, LANES), jnp.float32)
            for inside, block in blocks(number):
                value = block_of(inside, block)
                total = total + jnp.sum((value * value).reshape(-1, 8, LANES), axis=0)
            line[number, row : row + 1, :] = jnp.sum(total, axis=0, keepdims=True)

    def reduce(number):
        which, c = chunks[number]

        def total(inside, block):
            value = mean[which][block] + decode(got[which][(c, *inside)])
            mean[which][block] = value
            return value

        squares(number, 0, lambda inside, block: master[which][block])
        squares(number, 1, total)

    def turn(number):
        if axes[chunks[number][0]] == 0:
            for row in range(2):
                line[number, row : row + 1, :] = jnp.sum(
                    fold[number % 2, row].T, axis=0, keepdims=True
                )

    def send_line(number):
        for k in range(m - 1):
            line_copy(number, k).start()

    def ratio_of(number):
        both = line[number]
        for k in range(m - 1):
            both = both + line_got[number, k]
        own, slope = both[0:1], both[1:2]
        return jnp.sqrt(own) * lax.rsqrt(slope * rate**2 + 1e-06) * rate

    def wait_line(number):
        to_mate(line_got.at[number], line_got.at[number], line_recv.at[number], 0).wait_recv()

    def spread(number):
        tile[number % 2] = jnp.broadcast_to(ratio_of(number), (LANES, LANES)).T

    def update(number):
        which, c = chunks[number]
        axis = axes[which]
        share = mean[which].shape[axis]
        base = pl.multiple_of(me * share + c * LANES, LANES)
        if axis == 1:
            ratio = ratio_of(number)
        for inside, block in blocks(number):
            if axis == 0:
                scale = jnp.concatenate(
                    [tile[number % 2, inside[0], :]] * (mean[which].shape[1] // LANES), axis=1
                )
                first = inside[0].start
                target = (pl.ds(pl.multiple_of(base + first, 32), inside[0].size), slice(None))
            else:
                scale = ratio
                target = (inside[0], pl.ds(base, LANES))
            new = hold_rate * memory[which][block] + mean[which][block] * scale
            state[which][block] = new
            new = master[which][block] - learn_rate * new
            stepped[which][block] = new
            compute[which][target] = new.astype(jnp.bfloat16)

    def norm():
        for copy in norm_loads:
            copy.wait()
        part_norm_copy.wait()
        new = hold_rate * memory_n[...] + (mean_n[...] + got_n[...]) * rate
        state_norm[...] = new
        new = master_n[...] - learn_rate * new
        stepped_norm[...] = new
        whole_n[:, own_n] = new
        whole_norm_copy.start()

    barrier = pltpu.get_barrier_semaphore()

    def signal(target, **where):
        pl.semaphore_signal(target, inc=1, device_id=where, device_id_type=MESH)

    @pl.when(me == 0)
    def _():
        signal(barrier, replica=peer)
        for mate in mates:
            signal(barrier, model=mate)

    @pl.when(me == 1)
    def _():
        for mate in mates:
            signal(barrier, model=mate, replica=peer)

    for number in range(count + lead):
        if number < count:
            load(0, number).start()
        if number == lead:
            for copy in norm_loads:
                copy.start()
        if number + 1 >= lead and number + 1 - lead < count:
            load(2, number + 1 - lead).start()
            load(1, number + 1 - lead).start()

    @pl.when(me == 1)
    def _():
        pl.semaphore_wait(barrier, 1)
        signal(ready, replica=peer)

    @pl.when(me == 0)
    def _():
        pl.semaphore_wait(ready, 1)

    for number in range(lead):
        load(0, number).wait()
        prepare(number)
        part_copy(number).start()
    part_norm_copy.start()
    for number in range(count):
        wait_loads(number)
        part_copy(number).wait_recv()
        if number > 0:
            turn(number - 1)
        reduce(number)
        if number + lead < count:
            prepare(number + lead)
            part_copy(number + lead).start()
        load(3, number).start()
        if number == 0:

            @pl.when(me == 0)
            def _():
                pl.semaphore_wait(barrier, 2 * (m - 1))
                signal(ready, replica=peer)

            @pl.when(me == 1)
            def _():
                pl.semaphore_wait(ready, 1)

        if number > 0 and axes[chunks[number - 1][0]] == 0:
            send_line(number - 1)
        if axes[chunks[number][0]] == 1:
            send_line(number)
    if axes[chunks[-1][0]] == 0:
        turn(count - 1)
        send_line(count - 1)
    norm()

    for number in range(count):
        load(3, number).wait()
        wait_line(number)
        if axes[chunks[number][0]] == 0:
            spread(number)
        update(number)
        comp_copy(number).start()

    whole_norm_copy.wait()
    for j in range(whole_n.shape[1] // LANES):
        line_n[pl.ds(j, 1), :] = whole_n[:, j * LANES : (j + 1) * LANES]
    compute_norm[...] = line_n[...].astype(jnp.bfloat16)
    for which in range(t):
        to_peer(sent[which], got[which], part_send.at[which], part_recv.at[0]).wait_send()
        comp_half(which).wait()
    to_mate(line_got, line_got, line_recv.at[0], 0).wait_send()


def drain(*refs):
    half = len(refs) // 2
    sems = refs[-1]
    copies = [
        pltpu.make_async_copy(refs[i], refs[half + i], sems.at[i]) for i in range(half)
    ]
    for copy in copies:
        copy.start()
    for copy in copies:
        copy.wait()


def exchange(m, args):
    axes = (0, 0, 1)
    partial, partial_norm = args[0:3], args[3]
    master, master_norm = args[4:7], args[7]
    memory, memory_norm = args[8:11], args[11]
    row = lambda x: x.reshape(1, -1)
    shapes = [x.shape for x in master]
    counts = [s[a] // LANES for s, a in zip(shapes, axes)]
    pieces = [
        (c, LANES, s[1]) if a == 0 else (c, s[0], LANES)
        for s, a, c in zip(shapes, axes, counts)
    ]
    count = sum(counts)
    share_n, width_n = master_norm.shape[0], partial_norm.shape[1]
    f32, bf16 = jnp.float32, jnp.bfloat16
    dma = lambda *s: pltpu.SemaphoreType.DMA(s)
    out_shape = (
        [pltpu.VMEM(x.shape[1:], bf16) for x in partial]
        + [pltpu.VMEM((width_n // LANES, LANES), bf16)]
        + ([pltpu.VMEM(s, f32) for s in shapes] + [pltpu.VMEM((1, share_n), f32)]) * 2
    )
    scratch = (
        [pltpu.VMEM(s, f32) for s in shapes]
        + [pltpu.VMEM(s, bf16) for s in pieces] * 2
        + [pltpu.VMEM(s, f32) for s in shapes]
        + [pltpu.VMEM((1, share_n), f32)] * 4
        + [
            pltpu.VMEM((1, width_n), f32),
            pltpu.VMEM((width_n // LANES, LANES), f32),
            pltpu.VMEM((count, 2, LANES), f32),
            pltpu.VMEM((count, m - 1, 2, LANES), f32),
            pltpu.VMEM((2, 2, LANES, LANES), f32),
            pltpu.VMEM((2, LANES, LANES), f32),
            dma(count + 4),
            dma(len(shapes)),
            dma(count),
            dma(len(shapes)),
            dma(len(shapes)),
            dma(1),
            dma(count),
            dma(3),
            dma(2),
            dma(2),
            pltpu.SemaphoreType.REGULAR,
        ]
    )
    results = sum(math.prod(x.shape) * jnp.dtype(x.dtype).itemsize for x in out_shape)
    room = 63 * 2**20 - results
    outs = pl.pallas_call(
        functools.partial(kernel, m, axes),
        out_shape=out_shape,
        in_specs=[pl.BlockSpec(memory_space=pltpu.HBM)] * 12,
        out_specs=[pl.BlockSpec(memory_space=pltpu.VMEM)] * 12,
        scratch_shapes=scratch,
        compiler_params=pltpu.CompilerParams(
            collective_id=0, has_side_effects=True, vmem_limit_bytes=room
        ),
    )(
        *partial, partial_norm, *master, row(master_norm), *memory, row(memory_norm)
    )
    outs = pl.pallas_call(
        drain,
        out_shape=[jax.ShapeDtypeStruct(x.shape, x.dtype) for x in outs],
        in_specs=[pl.BlockSpec(memory_space=pl.ANY)] * len(outs),
        out_specs=[pl.BlockSpec(memory_space=pltpu.HBM)] * len(outs),
        scratch_shapes=[dma(len(outs))],
        compiler_params=pltpu.CompilerParams(vmem_limit_bytes=2**20),
    )(*outs)
    return [x.reshape(-1) if i % 4 == 3 else x for i, x in enumerate(outs)]


def plain(args):
    partial, master, memory = args[0:4], args[4:8], args[8:12]
    n = lax.axis_size("replica")
    axes = (0, 0, 1, 0)
    mean = [
        lax.psum_scatter(p[0], "replica", scatter_dimension=a, tiled=True) * n ** (-0.5)
        for p, a in zip(partial, axes)
    ]
    square = lambda x, a: jnp.sum(x * x, axis=1 - a, keepdims=True)
    own, slope = lax.psum(
        (
            [square(x, a) for x, a in zip(master[:3], axes)],
            [square(x, a) for x, a in zip(mean[:3], axes)],
        ),
        "model",
    )
    mean = [
        x * (jnp.sqrt(o) * lax.rsqrt(s + 1e-06)) for x, o, s in zip(mean[:3], own, slope)
    ] + mean[3:]
    state = [hold_rate * e + x for e, x in zip(memory, mean)]
    stepped = [w - learn_rate * s for w, s in zip(master, state)]
    compute = [
        lax.all_gather(s.astype(jnp.bfloat16), "replica", axis=a, tiled=True)
        for s, a in zip(stepped, axes)
    ]
    return compute + stepped + state


def on_device(*args):
    n, m = lax.axis_size("replica"), lax.axis_size("model")
    gate, up, down, gain = (x.shape for x in args[4:8])
    shares = (gate[0], up[0], down[1], gain[0])
    if (
        n == 2
        and m > 1
        and all(s % LANES == 0 and s >= 3 * LANES for s in shares)
        and gate[1] == up[1] == down[0]
    ):
        return tuple(exchange(m, args))
    return tuple(plain(args))


def solution(mesh):
    partial = P(("shift", "replica"), None, "model")
    rows, columns = P(("shift", "replica"), "model"), P(("shift", "model"), "replica")
    vector = P(("shift", "replica"))
    own = (rows, rows, columns, vector)
    return jax.shard_map(
        on_device,
        mesh=mesh,
        in_specs=(
            partial,
            partial,
            P(("shift", "replica"), "model", None),
            P(("shift", "replica"), None),
        )
        + own
        + own,
        out_specs=(
            P("shift", "model"),
            P("shift", "model"),
            P(("shift", "model"), None),
            P("shift"),
        )
        + own
        + own,
        check_vma=False,
    )
```

```python
import functools
import math

import jax
import jax.numpy as jnp
from jax import lax
from jax.experimental import pallas as pl
from jax.experimental.pallas import tpu as pltpu
from jax.sharding import PartitionSpec as P

learn_rate = 0.5
hold_rate = 0.9
MESH = pl.DeviceIdType.MESH
LANES = 128
CODE_SCALE = 2.0**13


def cut(ref, axis, start, size):
    return ref.at[pl.ds(start, size), :] if axis == 0 else ref.at[:, pl.ds(start, size)]


def code(x):
    x = x * CODE_SCALE
    x = x * x * x
    return (x * x * x).astype(jnp.bfloat16)


def decode(y):
    y = y.astype(jnp.float32)
    size = jnp.maximum(jnp.abs(y), 2.0**-126)
    return y * lax.exp2(lax.log2(size) * (-8 / 9) - math.log2(CODE_SCALE))


def kernel(m, axes, count, *refs):
    sems = lambda *shape: pltpu.SemaphoreType.DMA(shape)
    pl.run_scoped(
        functools.partial(body, m, axes, refs),
        sems(count + 8),
        sems(len(axes)),
        sems(count),
        sems(len(axes)),
        sems(1),
        sems(count),
        sems(1),
        sems(2),
        sems(2),
        pltpu.SemaphoreType.REGULAR,
    )


def body(m, axes, refs, load_sem, part_send, part_recv, comp_recv, *more):
    line_send, line_recv, norm_load_sem, norm_send, norm_recv, ready = more
    refs = list(refs)
    take = lambda count: [refs.pop(0) for _ in range(count)]
    t = len(axes)
    partial, (partial_norm,) = take(t), take(1)
    master_hbm, (master_norm,) = take(t), take(1)
    memory_hbm, (memory_norm,) = take(t), take(1)
    compute, (compute_norm,) = take(t), take(1)
    stepped, (stepped_norm,) = take(t), take(1)
    state, (state_norm,) = take(t), take(1)
    other, sent, got, memory = take(t), take(t), take(t), take(t)
    master, mean = stepped, state
    own_norm, got_n, whole_n, line_n = take(4)
    line, line_got, fold, tile = take(4)

    me = lax.axis_index("replica")
    at = lax.axis_index("model")
    peer = 1 - me
    rate = 2 ** (-0.5)
    mates = [lax.rem(at + k, m) for k in range(1, m)]

    chunks = []
    for which, axis in enumerate(axes):
        share = mean[which].shape[axis]
        chunks += [(which, c) for c in range(share // LANES)]
    for c in range(2):
        chunks.insert(c, chunks.pop(chunks.index((t - 1, c))))
    count, lead = len(chunks), 8

    def slot_of(kind, number):
        if kind == 0:
            return count + number if number < lead else number + 1 - lead
        return number

    def load(kind, number):
        which, c = chunks[number]
        axis = axes[which]
        share = mean[which].shape[axis]
        source = (partial[which].at[0], partial[which].at[0], master_hbm[which], memory_hbm[which])
        target = (other, mean, master, memory)[kind][which]
        start = ((peer, me)[kind] * share if kind < 2 else 0) + c * LANES
        start = pl.multiple_of(start, LANES)
        return pltpu.make_async_copy(
            cut(source[kind], axis, start, LANES),
            cut(target, axis, c * LANES, LANES),
            load_sem.at[slot_of(kind, number)],
        )

    def wait_loads(number):
        size = (3 if 0 < number <= count - lead else 2) * LANES
        pltpu.make_async_copy(
            master_hbm[0].at[pl.ds(0, size), :],
            master[0].at[pl.ds(0, size), :],
            load_sem.at[number],
        ).wait()

    share_n = got_n.shape[1]
    own_n = pl.ds(pl.multiple_of(me * share_n, LANES), share_n)
    norm_loads = [
        pltpu.make_async_copy(source, own_norm.at[i], norm_load_sem.at[0])
        for i, source in enumerate((partial_norm.at[:, own_n], master_norm, memory_norm))
    ]

    def to_peer(source, target, send, recv):
        return pltpu.make_async_remote_copy(
            src_ref=source,
            dst_ref=target,
            send_sem=send,
            recv_sem=recv,
            device_id={"replica": peer},
            device_id_type=MESH,
        )

    def part_copy(number):
        which, c = chunks[number]
        return to_peer(
            sent[which].at[c], got[which].at[c], part_send.at[which], part_recv.at[number]
        )

    def comp_copy(number):
        which, c = chunks[number]
        axis = axes[which]
        share = mean[which].shape[axis]
        mine = cut(compute[which], axis, pl.multiple_of(me * share + c * LANES, LANES), LANES)
        return to_peer(mine, mine, part_send.at[which], comp_recv.at[which])

    def comp_half(which):
        axis = axes[which]
        share = mean[which].shape[axis]
        mine = cut(compute[which], axis, pl.multiple_of(me * share, LANES), share)
        return to_peer(mine, mine, part_send.at[which], comp_recv.at[which])

    peer_n = pl.ds(pl.multiple_of(peer * share_n, LANES), share_n)
    part_norm_copy = to_peer(partial_norm.at[:, peer_n], got_n, norm_send.at[0], norm_recv.at[0])
    whole_norm_copy = to_peer(
        whole_n.at[:, own_n], whole_n.at[:, own_n], norm_send.at[1], norm_recv.at[1]
    )

    def to_mate(source, target, recv, k):
        return pltpu.make_async_remote_copy(
            src_ref=source,
            dst_ref=target,
            send_sem=line_send.at[0],
            recv_sem=recv,
            device_id={"model": mates[k]},
            device_id_type=MESH,
        )

    def line_copy(number, k):
        return to_mate(line.at[number], line_got.at[number, k], line_recv.at[number], k)

    def blocks(number):
        which, c = chunks[number]
        rows, columns = mean[which].shape
        if axes[which] == 0:
            height = 32
            for b in range(LANES // height):
                inside = (pl.ds(b * height, height), slice(None))
                yield inside, (pl.ds(c * LANES + b * height, height), slice(None))
        else:
            height = next(h for h in (128, 64, 32, 16, 8) if rows % h == 0)
            for b in range(rows // height):
                r = pl.ds(b * height, height)
                yield (r, slice(None)), (r, pl.ds(c * LANES, LANES))

    def prepare(number):
        which, c = chunks[number]
        for inside, block in blocks(number):
            sent[which][(c, *inside)] = code(other[which][block])

    def squares(number, row, block_of):
        which, c = chunks[number]
        if axes[which] == 0:
            for inside, block in blocks(number):
                value = block_of(inside, block)
                value = value * value
                fold[number % 2, row, inside[0], :] = sum(
                    value[:, j : j + LANES] for j in range(0, value.shape[1], LANES)
                )
        else:
            total = jnp.zeros((8, LANES), jnp.float32)
            for inside, block in blocks(number):
                value = block_of(inside, block)
                total = total + jnp.sum((value * value).reshape(-1, 8, LANES), axis=0)
            line[number, row : row + 1, :] = jnp.sum(total, axis=0, keepdims=True)

    def reduce(number):
        which, c = chunks[number]

        def total(inside, block):
            value = mean[which][block] + decode(got[which][(c, *inside)])
            mean[which][block] = value
            return value

        squares(number, 0, lambda inside, block: master[which][block])
        squares(number, 1, total)

    def turn(number):
        if axes[chunks[number][0]] == 0:
            for row in range(2):
                line[number, row : row + 1, :] = jnp.sum(
                    fold[number % 2, row].T, axis=0, keepdims=True
                )

    def send_line(number):
        for k in range(m - 1):
            line_copy(number, k).start()

    def ratio_of(number):
        both = line[number]
        for k in range(m - 1):
            both = both + line_got[number, k]
        own, slope = both[0:1], both[1:2]
        return jnp.sqrt(own) * lax.rsqrt(slope * rate**2 + 1e-06) * rate

    def wait_line(number):
        to_mate(line_got.at[number], line_got.at[number], line_recv.at[number], 0).wait_recv()

    def spread(number):
        tile[number % 2] = jnp.broadcast_to(ratio_of(number), (LANES, LANES)).T

    def update(number):
        which, c = chunks[number]
        axis = axes[which]
        share = mean[which].shape[axis]
        base = pl.multiple_of(me * share + c * LANES, LANES)
        if axis == 1:
            ratio = ratio_of(number)
        for inside, block in blocks(number):
            if axis == 0:
                scale = jnp.concatenate(
                    [tile[number % 2, inside[0], :]] * (mean[which].shape[1] // LANES), axis=1
                )
                first = inside[0].start
                target = (pl.ds(pl.multiple_of(base + first, 32), inside[0].size), slice(None))
            else:
                scale = ratio
                target = (inside[0], pl.ds(base, LANES))
            new = hold_rate * memory[which][block] + mean[which][block] * scale
            state[which][block] = new
            new = master[which][block] - learn_rate * new
            stepped[which][block] = new
            compute[which][target] = new.astype(jnp.bfloat16)

    def norm():
        pltpu.make_async_copy(own_norm, own_norm, norm_load_sem.at[0]).wait()
        part_norm_copy.wait()
        new = hold_rate * own_norm[2] + (own_norm[0] + got_n[...]) * rate
        state_norm[...] = new
        new = own_norm[1] - learn_rate * new
        stepped_norm[...] = new
        whole_n[:, own_n] = new
        whole_norm_copy.start()

    barrier = pltpu.get_barrier_semaphore()

    def signal(target, **where):
        pl.semaphore_signal(target, inc=1, device_id=where, device_id_type=MESH)

    for number in range(lead):
        load(0, number).start()
        if number == 2:
            load(2, 0).start()
            load(1, 0).start()

    @pl.when(me == 0)
    def _():
        signal(barrier, replica=peer)
        for mate in mates:
            signal(barrier, model=mate)

    @pl.when(me == 1)
    def _():
        for mate in mates:
            signal(barrier, model=mate, replica=peer)

    for number in range(count):
        if 0 < number <= count - lead:
            load(0, number + lead - 1).start()
        if number > 0:
            load(2, number).start()
            load(1, number).start()
        if number == 0:
            for copy in norm_loads:
                copy.start()

    @pl.when(me == 1)
    def _():
        pl.semaphore_wait(barrier, 1)
        signal(ready, replica=peer)

    @pl.when(me == 0)
    def _():
        pl.semaphore_wait(ready, 1)

    for number in range(lead):
        load(0, number).wait()
        prepare(number)
        part_copy(number).start()
    part_norm_copy.start()
    turned = 0
    for number in range(count):
        wait_loads(number)
        part_copy(number).wait_recv()
        ready_lines = [number] if axes[chunks[number][0]] == 1 else []
        if turned < number:
            turn(number - 1)
            ready_lines.insert(0, number - 1)
            turned = number
        reduce(number)
        if axes[chunks[number][0]] == 1:
            turned = number + 1
        if 0 < number <= count - lead:
            if turned == number:
                turn(number)
                ready_lines.append(number)
                turned = number + 1
            prepare(number + lead - 1)
            part_copy(number + lead - 1).start()
        for later in range(2 * (number - 6), 2 * (number - 5)):
            if 0 <= later < count:
                load(3, later).start()
        if number == 0:

            @pl.when(me == 0)
            def _():
                pl.semaphore_wait(barrier, 2 * (m - 1))
                signal(ready, replica=peer)

            @pl.when(me == 1)
            def _():
                pl.semaphore_wait(ready, 1)

        for done in ready_lines:
            send_line(done)
    if turned < count:
        turn(count - 1)
        send_line(count - 1)
    norm()
    for which in range(t):
        to_peer(sent[which], got[which], part_send.at[which], part_recv.at[0]).wait_send()

    for number in range(count):
        load(3, number).wait()
        wait_line(number)
        if axes[chunks[number][0]] == 0:
            spread(number)
        update(number)
        comp_copy(number).start()

    whole_norm_copy.wait()
    for j in range(whole_n.shape[1] // LANES):
        line_n[pl.ds(j, 1), :] = whole_n[:, j * LANES : (j + 1) * LANES]
    compute_norm[...] = line_n[...].astype(jnp.bfloat16)
    for which in range(t):
        comp_half(which).wait()
    to_mate(line_got, line_got, line_recv.at[0], 0).wait_send()


def drain(*refs):
    half = len(refs) // 2

    def run(sems):
        copies = [
            pltpu.make_async_copy(refs[i], refs[half + i], sems.at[i]) for i in range(half)
        ]
        for copy in copies:
            copy.start()
        for copy in copies:
            copy.wait()

    pl.run_scoped(run, pltpu.SemaphoreType.DMA((half,)))


def exchange(m, args):
    axes = (0, 0, 1)
    partial, partial_norm = args[0:3], args[3]
    master, master_norm = args[4:7], args[7]
    memory, memory_norm = args[8:11], args[11]
    row = lambda x: x.reshape(1, -1)
    shapes = [x.shape for x in master]
    counts = [s[a] // LANES for s, a in zip(shapes, axes)]
    pieces = [
        (c, LANES, s[1]) if a == 0 else (c, s[0], LANES)
        for s, a, c in zip(shapes, axes, counts)
    ]
    count = sum(counts)
    share_n, width_n = master_norm.shape[0], partial_norm.shape[1]
    f32, bf16 = jnp.float32, jnp.bfloat16
    out_shape = (
        [pltpu.VMEM(x.shape[1:], bf16) for x in partial]
        + [pltpu.VMEM((width_n // LANES, LANES), bf16)]
        + ([pltpu.VMEM(s, f32) for s in shapes] + [pltpu.VMEM((1, share_n), f32)]) * 2
    )
    scratch = (
        [pltpu.VMEM(s, f32) for s in shapes]
        + [pltpu.VMEM(s, bf16) for s in pieces] * 2
        + [pltpu.VMEM(s, f32) for s in shapes]
        + [
            pltpu.VMEM((3, 1, share_n), f32),
            pltpu.VMEM((1, share_n), f32),
            pltpu.VMEM((1, width_n), f32),
            pltpu.VMEM((width_n // LANES, LANES), f32),
            pltpu.VMEM((count, 2, LANES), f32),
            pltpu.VMEM((count, m - 1, 2, LANES), f32),
            pltpu.VMEM((2, 2, LANES, LANES), f32),
            pltpu.VMEM((2, LANES, LANES), f32),
        ]
    )
    results = sum(math.prod(x.shape) * jnp.dtype(x.dtype).itemsize for x in out_shape)
    room = 63 * 2**20 - results
    outs = pl.pallas_call(
        functools.partial(kernel, m, axes, count),
        out_shape=out_shape,
        in_specs=[pl.BlockSpec(memory_space=pltpu.HBM)] * 12,
        out_specs=[pl.BlockSpec(memory_space=pltpu.VMEM)] * 12,
        scratch_shapes=scratch,
        compiler_params=pltpu.CompilerParams(
            collective_id=0, has_side_effects=True, vmem_limit_bytes=room
        ),
    )(
        *partial, partial_norm, *master, row(master_norm), *memory, row(memory_norm)
    )
    outs = pl.pallas_call(
        drain,
        out_shape=[jax.ShapeDtypeStruct(x.shape, x.dtype) for x in outs],
        in_specs=[pl.BlockSpec(memory_space=pl.ANY)] * len(outs),
        out_specs=[pl.BlockSpec(memory_space=pltpu.HBM)] * len(outs),
        compiler_params=pltpu.CompilerParams(vmem_limit_bytes=2**20),
    )(*outs)
    return [x.reshape(-1) if i % 4 == 3 else x for i, x in enumerate(outs)]


def plain(args):
    partial, master, memory = args[0:4], args[4:8], args[8:12]
    n = lax.axis_size("replica")
    axes = (0, 0, 1, 0)
    mean = [
        lax.psum_scatter(p[0], "replica", scatter_dimension=a, tiled=True) * n ** (-0.5)
        for p, a in zip(partial, axes)
    ]
    square = lambda x, a: jnp.sum(x * x, axis=1 - a, keepdims=True)
    own, slope = lax.psum(
        (
            [square(x, a) for x, a in zip(master[:3], axes)],
            [square(x, a) for x, a in zip(mean[:3], axes)],
        ),
        "model",
    )
    mean = [
        x * (jnp.sqrt(o) * lax.rsqrt(s + 1e-06)) for x, o, s in zip(mean[:3], own, slope)
    ] + mean[3:]
    state = [hold_rate * e + x for e, x in zip(memory, mean)]
    stepped = [w - learn_rate * s for w, s in zip(master, state)]
    compute = [
        lax.all_gather(s.astype(jnp.bfloat16), "replica", axis=a, tiled=True)
        for s, a in zip(stepped, axes)
    ]
    return compute + stepped + state


def on_device(*args):
    n, m = lax.axis_size("replica"), lax.axis_size("model")
    gate, up, down, gain = (x.shape for x in args[4:8])
    shares = (gate[0], up[0], down[1], gain[0])
    if (
        n == 2
        and m > 1
        and all(s % LANES == 0 and s >= 3 * LANES for s in shares)
        and gate[1] == up[1] == down[0]
    ):
        return tuple(exchange(m, args))
    return tuple(plain(args))


def solution(mesh):
    partial = P(("shift", "replica"), None, "model")
    rows, columns = P(("shift", "replica"), "model"), P(("shift", "model"), "replica")
    vector = P(("shift", "replica"))
    own = (rows, rows, columns, vector)
    return jax.shard_map(
        on_device,
        mesh=mesh,
        in_specs=(
            partial,
            partial,
            P(("shift", "replica"), "model", None),
            P(("shift", "replica"), None),
        )
        + own
        + own,
        out_specs=(
            P("shift", "model"),
            P("shift", "model"),
            P(("shift", "model"), None),
            P("shift"),
        )
        + own
        + own,
        check_vma=False,
    )
```

```python
import functools
import math

import jax
import jax.numpy as jnp
from jax import lax
from jax.experimental import pallas as pl
from jax.experimental.pallas import tpu as pltpu
from jax.sharding import PartitionSpec as P

learn_rate = 0.5
hold_rate = 0.9
MESH = pl.DeviceIdType.MESH
LANES = 128
CODE_SCALE = 2.0**13
EXTRA = 2


def cut(ref, axis, start, size):
    return ref.at[pl.ds(start, size), :] if axis == 0 else ref.at[:, pl.ds(start, size)]


def code(x):
    x = x * CODE_SCALE
    x = x * x * x
    return (x * x * x).astype(jnp.bfloat16)


def decode(y):
    y = y.astype(jnp.float32)
    size = jnp.maximum(jnp.abs(y), 2.0**-126)
    return y * lax.exp2(lax.log2(size) * (-8 / 9) - math.log2(CODE_SCALE))


def kernel(m, axes, count, *refs):
    sems = lambda *shape: pltpu.SemaphoreType.DMA(shape)
    pl.run_scoped(
        functools.partial(body, m, axes, refs),
        sems(count + 8),
        sems(len(axes)),
        sems(count),
        sems(len(axes)),
        sems(1),
        sems(count),
        sems(1),
        sems(2),
        sems(2),
        pltpu.SemaphoreType.REGULAR,
        sems(EXTRA),
        sems(EXTRA),
        sems(1),
        sems(EXTRA),
    )


def body(m, axes, refs, load_sem, part_send, part_recv, comp_recv, *more):
    line_send, line_recv, norm_load_sem, norm_send, norm_recv, ready = more[:6]
    extra_send, extra_recv, cross_send, cross_recv = more[6:]
    refs = list(refs)
    take = lambda count: [refs.pop(0) for _ in range(count)]
    t = len(axes)
    partial, (partial_norm,) = take(t), take(1)
    master_hbm, (master_norm,) = take(t), take(1)
    memory_hbm, (memory_norm,) = take(t), take(1)
    compute, (compute_norm,) = take(t), take(1)
    stepped, (stepped_norm,) = take(t), take(1)
    state, (state_norm,) = take(t), take(1)
    other, sent, got, memory = take(t), take(t), take(t), take(t)
    master, mean = stepped, state
    own_norm, got_n, whole_n, line_n = take(4)
    line, line_got, fold, tile, extra, extra_got, cross = take(7)

    me = lax.axis_index("replica")
    at = lax.axis_index("model")
    peer = 1 - me
    rate = 2 ** (-0.5)
    mates = [lax.rem(at + k, m) for k in range(1, m)]

    chunks = []
    for which, axis in enumerate(axes):
        share = mean[which].shape[axis]
        chunks += [(which, c) for c in range(share // LANES)]
    for c in range(2):
        chunks.insert(c, chunks.pop(chunks.index((t - 1, c))))
    count, lead = len(chunks), 8

    def slot_of(kind, number):
        if kind == 0:
            return count + number if number < lead else number + 1 - lead
        return 2 * count - 1 - number if kind == 3 and number >= count - EXTRA else number

    def load(kind, number):
        which, c = chunks[number]
        axis = axes[which]
        share = mean[which].shape[axis]
        source = (partial[which].at[0], partial[which].at[0], master_hbm[which], memory_hbm[which])
        target = (other, mean, master, memory)[kind][which]
        start = ((peer, me)[kind] * share if kind < 2 else 0) + c * LANES
        start = pl.multiple_of(start, LANES)
        return pltpu.make_async_copy(
            cut(source[kind], axis, start, LANES),
            cut(target, axis, c * LANES, LANES),
            load_sem.at[slot_of(kind, number)],
        )

    def wait_loads(number):
        size = (3 if 0 < number <= count - lead else 2) * LANES
        pltpu.make_async_copy(
            master_hbm[0].at[pl.ds(0, size), :],
            master[0].at[pl.ds(0, size), :],
            load_sem.at[number],
        ).wait()

    share_n = got_n.shape[1]
    own_n = pl.ds(pl.multiple_of(me * share_n, LANES), share_n)
    norm_loads = [
        pltpu.make_async_copy(source, own_norm.at[i], norm_load_sem.at[0])
        for i, source in enumerate((partial_norm.at[:, own_n], master_norm, memory_norm))
    ]

    def to_peer(source, target, send, recv):
        return pltpu.make_async_remote_copy(
            src_ref=source,
            dst_ref=target,
            send_sem=send,
            recv_sem=recv,
            device_id={"replica": peer},
            device_id_type=MESH,
        )

    def part_copy(number):
        which, c = chunks[number]
        return to_peer(
            sent[which].at[c], got[which].at[c], part_send.at[which], part_recv.at[number]
        )

    def comp_copy(number):
        which, c = chunks[number]
        axis = axes[which]
        share = mean[which].shape[axis]
        mine = cut(compute[which], axis, pl.multiple_of(me * share + c * LANES, LANES), LANES)
        return to_peer(mine, mine, part_send.at[which], comp_recv.at[which])

    def comp_half(which):
        axis = axes[which]
        share = mean[which].shape[axis]
        size = share - EXTRA * LANES * (which == t - 1)
        mine = cut(compute[which], axis, pl.multiple_of(me * share, LANES), size)
        return to_peer(mine, mine, part_send.at[which], comp_recv.at[which])

    peer_n = pl.ds(pl.multiple_of(peer * share_n, LANES), share_n)
    part_norm_copy = to_peer(partial_norm.at[:, peer_n], got_n, norm_send.at[0], norm_recv.at[0])
    whole_norm_copy = to_peer(
        whole_n.at[:, own_n], whole_n.at[:, own_n], norm_send.at[1], norm_recv.at[1]
    )

    def to_mate(source, target, recv, k):
        return pltpu.make_async_remote_copy(
            src_ref=source,
            dst_ref=target,
            send_sem=line_send.at[0],
            recv_sem=recv,
            device_id={"model": mates[k]},
            device_id_type=MESH,
        )

    def line_copy(number, k):
        return to_mate(line.at[number], line_got.at[number, k], line_recv.at[number], k)

    first = count - EXTRA

    def extra_copy(number):
        x = number - first
        return to_peer(extra.at[x], extra_got.at[x], extra_send.at[x], extra_recv.at[x])

    def cross_copy(number, k):
        where = {"replica": peer} if k == 0 else {"model": mates[k - 1], "replica": peer}
        return pltpu.make_async_remote_copy(
            src_ref=line.at[number],
            dst_ref=cross.at[number - first, k],
            send_sem=cross_send.at[0],
            recv_sem=cross_recv.at[number - first],
            device_id=where,
            device_id_type=MESH,
        )

    def blocks(number):
        which, c = chunks[number]
        rows, columns = mean[which].shape
        if axes[which] == 0:
            height = 32
            for b in range(LANES // height):
                inside = (pl.ds(b * height, height), slice(None))
                yield inside, (pl.ds(c * LANES + b * height, height), slice(None))
        else:
            height = next(h for h in (128, 64, 32, 16, 8) if rows % h == 0)
            for b in range(rows // height):
                r = pl.ds(b * height, height)
                yield (r, slice(None)), (r, pl.ds(c * LANES, LANES))

    def prepare(number):
        which, c = chunks[number]
        for inside, block in blocks(number):
            sent[which][(c, *inside)] = code(other[which][block])

    def squares(number, row, block_of):
        which, c = chunks[number]
        if axes[which] == 0:
            for inside, block in blocks(number):
                value = block_of(inside, block)
                value = value * value
                fold[number % 2, row, inside[0], :] = sum(
                    value[:, j : j + LANES] for j in range(0, value.shape[1], LANES)
                )
        else:
            total = jnp.zeros((8, LANES), jnp.float32)
            for inside, block in blocks(number):
                value = block_of(inside, block)
                total = total + jnp.sum((value * value).reshape(-1, 8, LANES), axis=0)
            line[number, row : row + 1, :] = jnp.sum(total, axis=0, keepdims=True)

    def reduce(number):
        which, c = chunks[number]

        def total(inside, block):
            value = mean[which][block] + decode(got[which][(c, *inside)])
            mean[which][block] = value
            return value

        squares(number, 0, lambda inside, block: master[which][block])
        squares(number, 1, total)

    def turn(number):
        if axes[chunks[number][0]] == 0:
            for row in range(2):
                line[number, row : row + 1, :] = jnp.sum(
                    fold[number % 2, row].T, axis=0, keepdims=True
                )

    def send_line(number):
        for k in range(m - 1):
            line_copy(number, k).start()
        if number >= first:
            for k in range(m):
                cross_copy(number, k).start()

    def ratio_of(number):
        both = line[number]
        for k in range(m - 1):
            both = both + line_got[number, k]
        own, slope = both[0:1], both[1:2]
        return jnp.sqrt(own) * lax.rsqrt(slope * rate**2 + 1e-06) * rate

    def wait_line(number):
        to_mate(line_got.at[number], line_got.at[number], line_recv.at[number], 0).wait_recv()

    def spread(number):
        tile[number % 2] = jnp.broadcast_to(ratio_of(number), (LANES, LANES)).T

    def update(number):
        which, c = chunks[number]
        axis = axes[which]
        share = mean[which].shape[axis]
        base = pl.multiple_of(me * share + c * LANES, LANES)
        if axis == 1:
            ratio = ratio_of(number)
        for inside, block in blocks(number):
            if axis == 0:
                scale = jnp.concatenate(
                    [tile[number % 2, inside[0], :]] * (mean[which].shape[1] // LANES), axis=1
                )
                first = inside[0].start
                target = (pl.ds(pl.multiple_of(base + first, 32), inside[0].size), slice(None))
            else:
                scale = ratio
                target = (inside[0], pl.ds(base, LANES))
            new = hold_rate * memory[which][block] + mean[which][block] * scale
            state[which][block] = new
            new = master[which][block] - learn_rate * new
            stepped[which][block] = new
            compute[which][target] = new.astype(jnp.bfloat16)

    def pack(number):
        which, c = chunks[number]
        for inside, block in blocks(number):
            extra[(number - first, 0, *inside)] = code(mean[which][block])
            rest = master[which][block] - learn_rate * hold_rate * memory[which][block]
            extra[(number - first, 1, *inside)] = code(rest)

    def finish(number):
        which, c = chunks[number]
        x = number - first
        share = mean[which].shape[axes[which]]
        both = sum(cross[x, k] for k in range(m))
        scale = learn_rate * rate * jnp.sqrt(both[0:1])
        scale = scale * lax.rsqrt(both[1:2] * rate**2 + 1e-06)
        base = pl.multiple_of(peer * share + c * LANES, LANES)
        for inside, block in blocks(number):
            total = decode(extra_got[(x, 0, *inside)])
            rest = decode(extra_got[(x, 1, *inside)])
            compute[which][inside[0], pl.ds(base, LANES)] = (rest - total * scale).astype(jnp.bfloat16)

    def norm():
        pltpu.make_async_copy(own_norm, own_norm, norm_load_sem.at[0]).wait()
        part_norm_copy.wait()
        new = hold_rate * own_norm[2] + (own_norm[0] + got_n[...]) * rate
        state_norm[...] = new
        new = own_norm[1] - learn_rate * new
        stepped_norm[...] = new
        whole_n[:, own_n] = new
        whole_norm_copy.start()

    barrier = pltpu.get_barrier_semaphore()

    def signal(target, **where):
        pl.semaphore_signal(target, inc=1, device_id=where, device_id_type=MESH)

    for number in range(lead):
        load(0, number).start()
        if number == 2:
            load(2, 0).start()
            load(1, 0).start()

    @pl.when(me == 0)
    def _():
        signal(barrier, replica=peer)
        for mate in mates:
            signal(barrier, model=mate)

    @pl.when(me == 1)
    def _():
        for mate in mates:
            signal(barrier, model=mate, replica=peer)

    for number in range(count):
        if 0 < number <= count - lead:
            load(0, number + lead - 1).start()
        if number > 0:
            load(2, number).start()
            load(1, number).start()
        if number == 0:
            for copy in norm_loads:
                copy.start()

    @pl.when(me == 1)
    def _():
        pl.semaphore_wait(barrier, 1)
        signal(ready, replica=peer)

    @pl.when(me == 0)
    def _():
        pl.semaphore_wait(ready, 1)

    for number in range(lead):
        load(0, number).wait()
        prepare(number)
        part_copy(number).start()
    part_norm_copy.start()
    turned = 0
    for number in range(count):
        wait_loads(number)
        part_copy(number).wait_recv()
        ready_lines = [number] if axes[chunks[number][0]] == 1 else []
        if turned < number:
            turn(number - 1)
            ready_lines.insert(0, number - 1)
            turned = number
        reduce(number)
        if axes[chunks[number][0]] == 1:
            turned = number + 1
        if 0 < number <= count - lead:
            if turned == number:
                turn(number)
                ready_lines.append(number)
                turned = number + 1
            prepare(number + lead - 1)
            part_copy(number + lead - 1).start()
        for later in range(2 * (number - 6), 2 * (number - 5)):
            if 0 <= later < count:
                load(3, (later - EXTRA) % count).start()
        if number == 0:

            @pl.when(me == 0)
            def _():
                pl.semaphore_wait(barrier, 2 * (m - 1))
                signal(ready, replica=peer)

            @pl.when(me == 1)
            def _():
                pl.semaphore_wait(ready, 1)

        for done in ready_lines:
            send_line(done)
    if turned < count:
        turn(count - 1)
        send_line(count - 1)
    norm()
    for which in range(t):
        to_peer(sent[which], got[which], part_send.at[which], part_recv.at[0]).wait_send()

    for number in range(first, count):
        load(3, number).wait()
        pack(number)
        extra_copy(number).start()
    for number in range(count):
        if number < first:
            load(3, number).wait()
        wait_line(number)
        if axes[chunks[number][0]] == 0:
            spread(number)
        update(number)
        if number < first:
            comp_copy(number).start()

    for number in range(first, count):
        extra_copy(number).wait()
        arrived = cross.at[number - first]
        to_peer(arrived, arrived, cross_send.at[0], cross_recv.at[number - first]).wait_recv()
        finish(number)
    to_peer(cross, cross, cross_send.at[0], cross_recv.at[0]).wait_send()
    whole_norm_copy.wait()
    for j in range(whole_n.shape[1] // LANES):
        line_n[pl.ds(j, 1), :] = whole_n[:, j * LANES : (j + 1) * LANES]
    compute_norm[...] = line_n[...].astype(jnp.bfloat16)
    for which in range(t):
        comp_half(which).wait()
    to_mate(line_got, line_got, line_recv.at[0], 0).wait_send()


def drain(*refs):
    half = len(refs) // 2

    def run(sems):
        copies = [
            pltpu.make_async_copy(refs[i], refs[half + i], sems.at[i]) for i in range(half)
        ]
        for copy in copies:
            copy.start()
        for copy in copies:
            copy.wait()

    pl.run_scoped(run, pltpu.SemaphoreType.DMA((half,)))


def exchange(m, args):
    axes = (0, 0, 1)
    partial, partial_norm = args[0:3], args[3]
    master, master_norm = args[4:7], args[7]
    memory, memory_norm = args[8:11], args[11]
    row = lambda x: x.reshape(1, -1)
    shapes = [x.shape for x in master]
    counts = [s[a] // LANES for s, a in zip(shapes, axes)]
    pieces = [
        (c, LANES, s[1]) if a == 0 else (c, s[0], LANES)
        for s, a, c in zip(shapes, axes, counts)
    ]
    count = sum(counts)
    share_n, width_n = master_norm.shape[0], partial_norm.shape[1]
    f32, bf16 = jnp.float32, jnp.bfloat16
    out_shape = (
        [pltpu.VMEM(x.shape[1:], bf16) for x in partial]
        + [pltpu.VMEM((width_n // LANES, LANES), bf16)]
        + ([pltpu.VMEM(s, f32) for s in shapes] + [pltpu.VMEM((1, share_n), f32)]) * 2
    )
    scratch = (
        [pltpu.VMEM(s, f32) for s in shapes]
        + [pltpu.VMEM(s, bf16) for s in pieces] * 2
        + [pltpu.VMEM(s, f32) for s in shapes]
        + [
            pltpu.VMEM((3, 1, share_n), f32),
            pltpu.VMEM((1, share_n), f32),
            pltpu.VMEM((1, width_n), f32),
            pltpu.VMEM((width_n // LANES, LANES), f32),
            pltpu.VMEM((count, 2, LANES), f32),
            pltpu.VMEM((count, m - 1, 2, LANES), f32),
            pltpu.VMEM((2, 2, LANES, LANES), f32),
            pltpu.VMEM((2, LANES, LANES), f32),
            pltpu.VMEM((EXTRA, 2, shapes[-1][0], LANES), bf16),
            pltpu.VMEM((EXTRA, 2, shapes[-1][0], LANES), bf16),
            pltpu.VMEM((EXTRA, m, 2, LANES), f32),
        ]
    )
    results = sum(math.prod(x.shape) * jnp.dtype(x.dtype).itemsize for x in out_shape)
    room = 63 * 2**20 - results
    outs = pl.pallas_call(
        functools.partial(kernel, m, axes, count),
        out_shape=out_shape,
        in_specs=[pl.BlockSpec(memory_space=pltpu.HBM)] * 12,
        out_specs=[pl.BlockSpec(memory_space=pltpu.VMEM)] * 12,
        scratch_shapes=scratch,
        compiler_params=pltpu.CompilerParams(
            collective_id=0, has_side_effects=True, vmem_limit_bytes=room
        ),
    )(
        *partial, partial_norm, *master, row(master_norm), *memory, row(memory_norm)
    )
    outs = pl.pallas_call(
        drain,
        out_shape=[jax.ShapeDtypeStruct(x.shape, x.dtype) for x in outs],
        in_specs=[pl.BlockSpec(memory_space=pl.ANY)] * len(outs),
        out_specs=[pl.BlockSpec(memory_space=pltpu.HBM)] * len(outs),
        compiler_params=pltpu.CompilerParams(vmem_limit_bytes=2**20),
    )(*outs)
    return [x.reshape(-1) if i % 4 == 3 else x for i, x in enumerate(outs)]


def plain(args):
    partial, master, memory = args[0:4], args[4:8], args[8:12]
    n = lax.axis_size("replica")
    axes = (0, 0, 1, 0)
    mean = [
        lax.psum_scatter(p[0], "replica", scatter_dimension=a, tiled=True) * n ** (-0.5)
        for p, a in zip(partial, axes)
    ]
    square = lambda x, a: jnp.sum(x * x, axis=1 - a, keepdims=True)
    own, slope = lax.psum(
        (
            [square(x, a) for x, a in zip(master[:3], axes)],
            [square(x, a) for x, a in zip(mean[:3], axes)],
        ),
        "model",
    )
    mean = [
        x * (jnp.sqrt(o) * lax.rsqrt(s + 1e-06)) for x, o, s in zip(mean[:3], own, slope)
    ] + mean[3:]
    state = [hold_rate * e + x for e, x in zip(memory, mean)]
    stepped = [w - learn_rate * s for w, s in zip(master, state)]
    compute = [
        lax.all_gather(s.astype(jnp.bfloat16), "replica", axis=a, tiled=True)
        for s, a in zip(stepped, axes)
    ]
    return compute + stepped + state


def on_device(*args):
    n, m = lax.axis_size("replica"), lax.axis_size("model")
    gate, up, down, gain = (x.shape for x in args[4:8])
    shares = (gate[0], up[0], down[1], gain[0])
    if (
        n == 2
        and m > 1
        and all(s % LANES == 0 and s >= 3 * LANES for s in shares)
        and gate[1] == up[1] == down[0]
    ):
        return tuple(exchange(m, args))
    return tuple(plain(args))


def solution(mesh):
    partial = P(("shift", "replica"), None, "model")
    rows, columns = P(("shift", "replica"), "model"), P(("shift", "model"), "replica")
    vector = P(("shift", "replica"))
    own = (rows, rows, columns, vector)
    return jax.shard_map(
        on_device,
        mesh=mesh,
        in_specs=(
            partial,
            partial,
            P(("shift", "replica"), "model", None),
            P(("shift", "replica"), None),
        )
        + own
        + own,
        out_specs=(
            P("shift", "model"),
            P("shift", "model"),
            P(("shift", "model"), None),
            P("shift"),
        )
        + own
        + own,
        check_vma=False,
    )
```

```python
import functools
import math

import jax
import jax.numpy as jnp
from jax import lax
from jax.experimental import pallas as pl
from jax.experimental.pallas import tpu as pltpu
from jax.sharding import PartitionSpec as P

learn_rate = 0.5
hold_rate = 0.9
MESH = pl.DeviceIdType.MESH
LANES = 128
CODE_SCALE = 2.0**13
EXTRA = 2


def cut(ref, axis, start, size):
    return ref.at[pl.ds(start, size), :] if axis == 0 else ref.at[:, pl.ds(start, size)]


def code(x):
    x = x * CODE_SCALE
    x = x * x * x
    return (x * x * x).astype(jnp.bfloat16)


def decode(y):
    y = y.astype(jnp.float32)
    size = jnp.maximum(jnp.abs(y), 2.0**-126)
    return y * lax.exp2(lax.log2(size) * (-8 / 9) - math.log2(CODE_SCALE))


def kernel(m, axes, count, *refs):
    sems = lambda *shape: pltpu.SemaphoreType.DMA(shape)
    pl.run_scoped(
        functools.partial(body, m, axes, refs),
        sems(count + 8),
        sems(len(axes)),
        sems(count),
        sems(len(axes)),
        sems(1),
        sems(count),
        sems(1),
        sems(2),
        sems(2),
        pltpu.SemaphoreType.REGULAR,
        sems(EXTRA),
        sems(EXTRA),
        sems(1),
        sems(EXTRA),
    )


def body(m, axes, refs, load_sem, part_send, part_recv, comp_recv, *more):
    line_send, line_recv, norm_load_sem, norm_send, norm_recv, ready = more[:6]
    extra_send, extra_recv, cross_send, cross_recv = more[6:]
    refs = list(refs)
    take = lambda count: [refs.pop(0) for _ in range(count)]
    t = len(axes)
    partial, (partial_norm,) = take(t), take(1)
    master_hbm, (master_norm,) = take(t), take(1)
    memory_hbm, (memory_norm,) = take(t), take(1)
    compute, (compute_norm,) = take(t), take(1)
    stepped, (stepped_norm,) = take(t), take(1)
    state, (state_norm,) = take(t), take(1)
    other, sent, got, memory = take(t), take(t), take(t), take(t)
    master, mean = stepped, state
    own_norm, got_n, whole_n, line_n = take(4)
    line, line_got, fold, tile, extra, extra_got, cross = take(7)

    me = lax.axis_index("replica")
    at = lax.axis_index("model")
    peer = 1 - me
    rate = 2 ** (-0.5)
    mates = [lax.rem(at + k, m) for k in range(1, m)]

    chunks = []
    for which, axis in enumerate(axes):
        share = mean[which].shape[axis]
        chunks += [(which, c) for c in range(share // LANES)]
    for c in range(2):
        chunks.insert(c, chunks.pop(chunks.index((t - 1, c))))
    count, lead = len(chunks), 6

    def slot_of(kind, number):
        if kind == 0:
            return count + number if number < lead else number + 1 - lead
        return 2 * count - 1 - number if kind == 3 and number >= count - EXTRA else number

    def load(kind, number):
        which, c = chunks[number]
        axis = axes[which]
        share = mean[which].shape[axis]
        source = (partial[which].at[0], partial[which].at[0], master_hbm[which], memory_hbm[which])
        target = (other, mean, master, memory)[kind][which]
        start = ((peer, me)[kind] * share if kind < 2 else 0) + c * LANES
        start = pl.multiple_of(start, LANES)
        return pltpu.make_async_copy(
            cut(source[kind], axis, start, LANES),
            cut(target, axis, c * LANES, LANES),
            load_sem.at[slot_of(kind, number)],
        )

    def wait_loads(number):
        size = (3 if 0 < number <= count - lead else 2) * LANES
        pltpu.make_async_copy(
            master_hbm[0].at[pl.ds(0, size), :],
            master[0].at[pl.ds(0, size), :],
            load_sem.at[number],
        ).wait()

    share_n = got_n.shape[1]
    own_n = pl.ds(pl.multiple_of(me * share_n, LANES), share_n)
    norm_loads = [
        pltpu.make_async_copy(source, own_norm.at[i], norm_load_sem.at[0])
        for i, source in enumerate((partial_norm.at[:, own_n], master_norm, memory_norm))
    ]

    def to_peer(source, target, send, recv):
        return pltpu.make_async_remote_copy(
            src_ref=source,
            dst_ref=target,
            send_sem=send,
            recv_sem=recv,
            device_id={"replica": peer},
            device_id_type=MESH,
        )

    def part_copy(number):
        which, c = chunks[number]
        return to_peer(
            sent[which].at[c], got[which].at[c], part_send.at[which], part_recv.at[number]
        )

    def comp_copy(number):
        which, c = chunks[number]
        axis = axes[which]
        share = mean[which].shape[axis]
        mine = cut(compute[which], axis, pl.multiple_of(me * share + c * LANES, LANES), LANES)
        return to_peer(mine, mine, part_send.at[which], comp_recv.at[which])

    def comp_half(which):
        axis = axes[which]
        share = mean[which].shape[axis]
        size = share - EXTRA * LANES * (which == t - 1)
        mine = cut(compute[which], axis, pl.multiple_of(me * share, LANES), size)
        return to_peer(mine, mine, part_send.at[which], comp_recv.at[which])

    peer_n = pl.ds(pl.multiple_of(peer * share_n, LANES), share_n)
    part_norm_copy = to_peer(partial_norm.at[:, peer_n], got_n, norm_send.at[0], norm_recv.at[0])
    whole_norm_copy = to_peer(
        whole_n.at[:, own_n], whole_n.at[:, own_n], norm_send.at[1], norm_recv.at[1]
    )

    def to_mate(source, target, recv, k):
        return pltpu.make_async_remote_copy(
            src_ref=source,
            dst_ref=target,
            send_sem=line_send.at[0],
            recv_sem=recv,
            device_id={"model": mates[k]},
            device_id_type=MESH,
        )

    def line_copy(number, k):
        return to_mate(line.at[number], line_got.at[number, k], line_recv.at[number], k)

    first = count - EXTRA

    def extra_copy(number):
        x = number - first
        return to_peer(extra.at[x], extra_got.at[x], extra_send.at[x], extra_recv.at[x])

    def cross_copy(number, k):
        where = {"replica": peer} if k == 0 else {"model": mates[k - 1], "replica": peer}
        return pltpu.make_async_remote_copy(
            src_ref=line.at[number],
            dst_ref=cross.at[number - first, k],
            send_sem=cross_send.at[0],
            recv_sem=cross_recv.at[number - first],
            device_id=where,
            device_id_type=MESH,
        )

    def blocks(number):
        which, c = chunks[number]
        rows, columns = mean[which].shape
        if axes[which] == 0:
            height = 32
            for b in range(LANES // height):
                inside = (pl.ds(b * height, height), slice(None))
                yield inside, (pl.ds(c * LANES + b * height, height), slice(None))
        else:
            height = next(h for h in (128, 64, 32, 16, 8) if rows % h == 0)
            for b in range(rows // height):
                r = pl.ds(b * height, height)
                yield (r, slice(None)), (r, pl.ds(c * LANES, LANES))

    def prepare(number):
        which, c = chunks[number]
        for inside, block in blocks(number):
            sent[which][(c, *inside)] = code(other[which][block])

    def squares(number, row, block_of):
        which, c = chunks[number]
        if axes[which] == 0:
            for inside, block in blocks(number):
                value = block_of(inside, block)
                value = value * value
                fold[number % 2, row, inside[0], :] = sum(
                    value[:, j : j + LANES] for j in range(0, value.shape[1], LANES)
                )
        else:
            total = jnp.zeros((8, LANES), jnp.float32)
            for inside, block in blocks(number):
                value = block_of(inside, block)
                total = total + jnp.sum((value * value).reshape(-1, 8, LANES), axis=0)
            line[number, row : row + 1, :] = jnp.sum(total, axis=0, keepdims=True)

    def reduce(number):
        which, c = chunks[number]

        def total(inside, block):
            value = mean[which][block] + decode(got[which][(c, *inside)])
            mean[which][block] = value
            return value

        squares(number, 0, lambda inside, block: master[which][block])
        squares(number, 1, total)

    def turn(number):
        if axes[chunks[number][0]] == 0:
            for row in range(2):
                line[number, row : row + 1, :] = jnp.sum(
                    fold[number % 2, row].T, axis=0, keepdims=True
                )

    def send_line(number):
        for k in range(m - 1):
            line_copy(number, k).start()
        if number >= first:
            for k in range(m):
                cross_copy(number, k).start()

    def ratio_of(number):
        both = line[number]
        for k in range(m - 1):
            both = both + line_got[number, k]
        own, slope = both[0:1], both[1:2]
        return jnp.sqrt(own) * lax.rsqrt(slope * rate**2 + 1e-06) * rate

    def wait_line(number):
        to_mate(line_got.at[number], line_got.at[number], line_recv.at[number], 0).wait_recv()

    def spread(number):
        tile[number % 2] = jnp.broadcast_to(ratio_of(number), (LANES, LANES)).T

    def update(number):
        which, c = chunks[number]
        axis = axes[which]
        share = mean[which].shape[axis]
        base = pl.multiple_of(me * share + c * LANES, LANES)
        if axis == 1:
            ratio = ratio_of(number)
        for inside, block in blocks(number):
            if axis == 0:
                scale = jnp.concatenate(
                    [tile[number % 2, inside[0], :]] * (mean[which].shape[1] // LANES), axis=1
                )
                first = inside[0].start
                target = (pl.ds(pl.multiple_of(base + first, 32), inside[0].size), slice(None))
            else:
                scale = ratio
                target = (inside[0], pl.ds(base, LANES))
            new = hold_rate * memory[which][block] + mean[which][block] * scale
            state[which][block] = new
            new = master[which][block] - learn_rate * new
            stepped[which][block] = new
            compute[which][target] = new.astype(jnp.bfloat16)

    def pack(number):
        which, c = chunks[number]
        for inside, block in blocks(number):
            extra[(number - first, 0, *inside)] = code(mean[which][block])
            rest = master[which][block] - learn_rate * hold_rate * memory[which][block]
            extra[(number - first, 1, *inside)] = code(rest)

    def finish(number):
        which, c = chunks[number]
        x = number - first
        share = mean[which].shape[axes[which]]
        both = sum(cross[x, k] for k in range(m))
        scale = learn_rate * rate * jnp.sqrt(both[0:1])
        scale = scale * lax.rsqrt(both[1:2] * rate**2 + 1e-06)
        base = pl.multiple_of(peer * share + c * LANES, LANES)
        for inside, block in blocks(number):
            total = decode(extra_got[(x, 0, *inside)])
            rest = decode(extra_got[(x, 1, *inside)])
            compute[which][inside[0], pl.ds(base, LANES)] = (rest - total * scale).astype(jnp.bfloat16)

    def norm():
        pltpu.make_async_copy(own_norm, own_norm, norm_load_sem.at[0]).wait()
        part_norm_copy.wait()
        new = hold_rate * own_norm[2] + (own_norm[0] + got_n[...]) * rate
        state_norm[...] = new
        new = own_norm[1] - learn_rate * new
        stepped_norm[...] = new
        whole_n[:, own_n] = new
        whole_norm_copy.start()

    barrier = pltpu.get_barrier_semaphore()

    def signal(target, **where):
        pl.semaphore_signal(target, inc=1, device_id=where, device_id_type=MESH)

    for number in range(lead):
        load(0, number).start()
        if number == 2:
            load(2, 0).start()
            load(1, 0).start()

    @pl.when(me == 0)
    def _():
        signal(barrier, replica=peer)
        for mate in mates:
            signal(barrier, model=mate)

    @pl.when(me == 1)
    def _():
        for mate in mates:
            signal(barrier, model=mate, replica=peer)

    for number in range(count):
        if 0 < number <= count - lead:
            load(0, number + lead - 1).start()
        if number > 0:
            load(2, number).start()
            load(1, number).start()
        if number == 0:
            for copy in norm_loads:
                copy.start()

    @pl.when(me == 1)
    def _():
        pl.semaphore_wait(barrier, 1)
        signal(ready, replica=peer)

    @pl.when(me == 0)
    def _():
        pl.semaphore_wait(ready, 1)

    for number in range(lead):
        load(0, number).wait()
        prepare(number)
        part_copy(number).start()
    part_norm_copy.start()
    turned = 0
    for number in range(count):
        wait_loads(number)
        part_copy(number).wait_recv()
        ready_lines = [number] if axes[chunks[number][0]] == 1 else []
        if turned < number:
            turn(number - 1)
            ready_lines.insert(0, number - 1)
            turned = number
        reduce(number)
        if axes[chunks[number][0]] == 1:
            turned = number + 1
        if 0 < number <= count - lead:
            if turned == number:
                turn(number)
                ready_lines.append(number)
                turned = number + 1
            prepare(number + lead - 1)
            part_copy(number + lead - 1).start()
        for later in range(2 * (number - 6), 2 * (number - 5)):
            if 0 <= later < count:
                load(3, (later - EXTRA) % count).start()
        if number == 0:

            @pl.when(me == 0)
            def _():
                pl.semaphore_wait(barrier, 2 * (m - 1))
                signal(ready, replica=peer)

            @pl.when(me == 1)
            def _():
                pl.semaphore_wait(ready, 1)

        for done in ready_lines:
            send_line(done)
    if turned < count:
        turn(count - 1)
        send_line(count - 1)
    norm()
    for which in range(t):
        to_peer(sent[which], got[which], part_send.at[which], part_recv.at[0]).wait_send()

    for number in range(first, count):
        load(3, number).wait()
        pack(number)
        extra_copy(number).start()
    for number in range(count):
        if number < first:
            load(3, number).wait()
        wait_line(number)
        if axes[chunks[number][0]] == 0:
            spread(number)
        update(number)
        if number < first:
            comp_copy(number).start()

    for number in range(first, count):
        extra_copy(number).wait()
        arrived = cross.at[number - first]
        to_peer(arrived, arrived, cross_send.at[0], cross_recv.at[number - first]).wait_recv()
        finish(number)
    to_peer(cross, cross, cross_send.at[0], cross_recv.at[0]).wait_send()
    whole_norm_copy.wait()
    for j in range(whole_n.shape[1] // LANES):
        line_n[pl.ds(j, 1), :] = whole_n[:, j * LANES : (j + 1) * LANES]
    compute_norm[...] = line_n[...].astype(jnp.bfloat16)
    for which in range(t):
        comp_half(which).wait()
    to_mate(line_got, line_got, line_recv.at[0], 0).wait_send()


def drain(*refs):
    half = len(refs) // 2

    def run(sems):
        copies = [
            pltpu.make_async_copy(refs[i], refs[half + i], sems.at[i]) for i in range(half)
        ]
        for copy in copies:
            copy.start()
        for copy in copies:
            copy.wait()

    pl.run_scoped(run, pltpu.SemaphoreType.DMA((half,)))


def exchange(m, args):
    axes = (0, 0, 1)
    partial, partial_norm = args[0:3], args[3]
    master, master_norm = args[4:7], args[7]
    memory, memory_norm = args[8:11], args[11]
    row = lambda x: x.reshape(1, -1)
    shapes = [x.shape for x in master]
    counts = [s[a] // LANES for s, a in zip(shapes, axes)]
    pieces = [
        (c, LANES, s[1]) if a == 0 else (c, s[0], LANES)
        for s, a, c in zip(shapes, axes, counts)
    ]
    count = sum(counts)
    share_n, width_n = master_norm.shape[0], partial_norm.shape[1]
    f32, bf16 = jnp.float32, jnp.bfloat16
    out_shape = (
        [pltpu.VMEM(x.shape[1:], bf16) for x in partial]
        + [pltpu.VMEM((width_n // LANES, LANES), bf16)]
        + ([pltpu.VMEM(s, f32) for s in shapes] + [pltpu.VMEM((1, share_n), f32)]) * 2
    )
    scratch = (
        [pltpu.VMEM(s, f32) for s in shapes]
        + [pltpu.VMEM(s, bf16) for s in pieces] * 2
        + [pltpu.VMEM(s, f32) for s in shapes]
        + [
            pltpu.VMEM((3, 1, share_n), f32),
            pltpu.VMEM((1, share_n), f32),
            pltpu.VMEM((1, width_n), f32),
            pltpu.VMEM((width_n // LANES, LANES), f32),
            pltpu.VMEM((count, 2, LANES), f32),
            pltpu.VMEM((count, m - 1, 2, LANES), f32),
            pltpu.VMEM((2, 2, LANES, LANES), f32),
            pltpu.VMEM((2, LANES, LANES), f32),
            pltpu.VMEM((EXTRA, 2, shapes[-1][0], LANES), bf16),
            pltpu.VMEM((EXTRA, 2, shapes[-1][0], LANES), bf16),
            pltpu.VMEM((EXTRA, m, 2, LANES), f32),
        ]
    )
    results = sum(math.prod(x.shape) * jnp.dtype(x.dtype).itemsize for x in out_shape)
    room = 63 * 2**20 - results
    outs = pl.pallas_call(
        functools.partial(kernel, m, axes, count),
        out_shape=out_shape,
        in_specs=[pl.BlockSpec(memory_space=pltpu.HBM)] * 12,
        out_specs=[pl.BlockSpec(memory_space=pltpu.VMEM)] * 12,
        scratch_shapes=scratch,
        compiler_params=pltpu.CompilerParams(
            collective_id=0, has_side_effects=True, vmem_limit_bytes=room
        ),
    )(
        *partial, partial_norm, *master, row(master_norm), *memory, row(memory_norm)
    )
    outs = pl.pallas_call(
        drain,
        out_shape=[jax.ShapeDtypeStruct(x.shape, x.dtype) for x in outs],
        in_specs=[pl.BlockSpec(memory_space=pl.ANY)] * len(outs),
        out_specs=[pl.BlockSpec(memory_space=pltpu.HBM)] * len(outs),
        compiler_params=pltpu.CompilerParams(vmem_limit_bytes=2**20),
    )(*outs)
    return [x.reshape(-1) if i % 4 == 3 else x for i, x in enumerate(outs)]


def plain(args):
    partial, master, memory = args[0:4], args[4:8], args[8:12]
    n = lax.axis_size("replica")
    axes = (0, 0, 1, 0)
    mean = [
        lax.psum_scatter(p[0], "replica", scatter_dimension=a, tiled=True) * n ** (-0.5)
        for p, a in zip(partial, axes)
    ]
    square = lambda x, a: jnp.sum(x * x, axis=1 - a, keepdims=True)
    own, slope = lax.psum(
        (
            [square(x, a) for x, a in zip(master[:3], axes)],
            [square(x, a) for x, a in zip(mean[:3], axes)],
        ),
        "model",
    )
    mean = [
        x * (jnp.sqrt(o) * lax.rsqrt(s + 1e-06)) for x, o, s in zip(mean[:3], own, slope)
    ] + mean[3:]
    state = [hold_rate * e + x for e, x in zip(memory, mean)]
    stepped = [w - learn_rate * s for w, s in zip(master, state)]
    compute = [
        lax.all_gather(s.astype(jnp.bfloat16), "replica", axis=a, tiled=True)
        for s, a in zip(stepped, axes)
    ]
    return compute + stepped + state


def on_device(*args):
    n, m = lax.axis_size("replica"), lax.axis_size("model")
    gate, up, down, gain = (x.shape for x in args[4:8])
    shares = (gate[0], up[0], down[1], gain[0])
    if (
        n == 2
        and m > 1
        and all(s % LANES == 0 and s >= 3 * LANES for s in shares)
        and gate[1] == up[1] == down[0]
    ):
        return tuple(exchange(m, args))
    return tuple(plain(args))


def solution(mesh):
    partial = P(("shift", "replica"), None, "model")
    rows, columns = P(("shift", "replica"), "model"), P(("shift", "model"), "replica")
    vector = P(("shift", "replica"))
    own = (rows, rows, columns, vector)
    return jax.shard_map(
        on_device,
        mesh=mesh,
        in_specs=(
            partial,
            partial,
            P(("shift", "replica"), "model", None),
            P(("shift", "replica"), None),
        )
        + own
        + own,
        out_specs=(
            P("shift", "model"),
            P("shift", "model"),
            P(("shift", "model"), None),
            P("shift"),
        )
        + own
        + own,
        check_vma=False,
    )
```
